32 devices in a mesh: aux: 4 (over x, core), row: 8 (over z, y).
Axes of the slice: x: 2, y: 2, z: 4, core: 2. Of those that a mesh axis runs over, the one named last changes fastest.
Arguments:
- integrals: bfloat16 [4, 8192, 8192], P('aux', 'row'), may hold values from -6 to 6
- orbitals: bfloat16 [8192, 768], P('row'), may hold values from -0.0011901855 to 0.0011901855
Outputs:
- exchange_matrix: float32 [8192, 8192], P('row', 'aux')
The draws below stay inside these ranges and needn't reach their ends.
All inputs are finite; a program needn't handle non-finite values.
Results may differ from the reference program's by a relative error of at most 0.0033.
Values may be sent and summed in bfloat16 or wider, within the bound.
A program may use at most 128 MiB of HBM per device.

```python
import jax
import jax.numpy as jnp

N = 8192
OCC = 768
NAUX = 4


def levels(stream_key, shape, pieces, smallest, largest):
    gain = 1.0
    for position, parts in pieces:
        steps = jax.random.uniform(jax.random.fold_in(jax.random.fold_in(stream_key, 6), position), (parts,), jnp.float32, smallest / len(pieces), largest / len(pieces))
        gain = gain * jnp.repeat(jnp.exp(steps), shape[position] // parts).reshape((-1,) + (1,) * (len(shape) - 1 - position))
    return gain


def normal_values(rng, dims, spread, limit, cuts=(), dtype=jnp.bfloat16):
    values = spread * jax.random.normal(rng, dims, jnp.float32)
    if cuts:
        values = values * levels(rng, dims, cuts, -0.22, 0.18)
    return jnp.clip(values, -limit, limit).astype(dtype)


def setup_inputs(seed: int = 0) -> dict:
    arg_keys = jax.random.split(jax.random.key(seed), 3)
    return {
        "integrals": normal_values(arg_keys[0], (NAUX, N, N), 1.0, 6.0, ((0, 4), (1, 8))),
        "orbitals": normal_values(arg_keys[1], (N, OCC), ((N * NAUX * OCC) ** -0.5), 0.0011901855, ((0, 8),)),
    }


def reference(integrals, orbitals):
    halves = []
    for index in range(NAUX):
        product = jnp.dot(integrals[index], orbitals, preferred_element_type=jnp.float32)
        halves.append(product.astype(jnp.bfloat16))
    joined = jnp.concatenate(halves, axis=1)
    return jnp.dot(joined, joined.T, preferred_element_type=jnp.float32)
```

```python
import jax
import jax.numpy as jnp
from jax import lax
from jax.sharding import PartitionSpec as P


def gather_orbitals(orbitals):
    rows = orbitals.shape[0] // lax.axis_size("aux")
    share = lax.dynamic_slice_in_dim(orbitals, lax.axis_index("aux") * rows, rows, axis=0)
    return lax.all_gather(share, ("row", "aux"), axis=0, tiled=True)


def column_halves(own_half):
    aux, row = lax.axis_size("aux"), lax.axis_size("row")
    span = row // aux
    moves = [
        (p * row + r, (r // span) * row + p * span + r % span)
        for p in range(aux)
        for r in range(row)
    ]
    moved = lax.ppermute(own_half, ("aux", "row"), moves)
    gathered = lax.all_gather(moved, "row", axis=0, tiled=False)
    parts = gathered.reshape((aux, span) + own_half.shape)
    parts = jnp.moveaxis(parts, 2, 1)
    return parts.reshape(aux * own_half.shape[0], span * own_half.shape[1], own_half.shape[2])


def body(integrals, orbitals):
    transformed = jnp.einsum(
        "arn,no->aro",
        integrals,
        gather_orbitals(orbitals),
        preferred_element_type=jnp.float32,
    )
    own_half = transformed.astype(jnp.bfloat16)
    columns = column_halves(own_half)
    rows = lax.all_gather(own_half, "aux", axis=0, tiled=True)
    return jnp.einsum("aro,aco->rc", rows, columns, preferred_element_type=jnp.float32)


def solution(mesh):
    in_specs = (P("aux", "row", None), P("row", None))
    out_specs = P("row", "aux")
    return jax.shard_map(body, mesh=mesh, in_specs=in_specs, out_specs=out_specs, check_vma=False)
```
